16 devices in a mesh: dp: 2 (over y, z), vp: 8 (over x, core).
Axes of the slice: x: 4, y: 2, z: 1, core: 2. Of those that a mesh axis runs over, the one named last changes fastest.
The devices are a block of a 4x4x8 slice.
Arguments:
- hidden: bfloat16 [4096, 4096], P(('dp', 'vp')), parts along dimension 0
- labels: int32 [4096], P(('dp', 'vp')), parts along dimension 0
- loss_weight: float32 [4096], P(('dp', 'vp')), parts along dimension 0
- norm_gain: float32 [4096], replicated
- w_unembed: bfloat16 [4096, 32896], P(None, 'vp')
Outputs:
- output 1: float32 [2], P('dp'), parts along dimension 0
- output 2: bfloat16 [4096, 4096], P(('dp', 'vp')), parts along dimension 0
- output 3: float32 [8192, 32896], P('dp', 'vp'), parts along dimension 0
- output 4: float32 [8192], P('dp'), parts along dimension 0
There are 2 independent parts. The reference program is written for one: setup_inputs(seed, part) draws one part's arguments, and reference() takes and returns one part's arrays. A program takes and returns all parts, laid end to end along the dimension named above; an argument that names none is the same for every part.
All inputs are finite; a program needn't handle non-finite values.
Results may differ from the reference program's by a relative error of at most 0.001.
Values are sent between devices in bfloat16 or wider.
A program may use at most 768 MiB of HBM per device.

```python
import jax
import jax.numpy as jnp
from jax import lax

D = 4096
V = 32768
PAD_COLS = 128
TOK_DEV = 256
GROUP_SIZE = 8
VOCAB_PAD = V + PAD_COLS
TOKENS = TOK_DEV * GROUP_SIZE
LOW_IDS = V // 64
NORM_EPS = 1e-5


def setup_inputs(seed: int = 0, part: int = 0) -> dict:
    base_key = jax.random.key(seed)
    shared_key, parts_key = jax.random.split(base_key)
    part_key = jax.random.fold_in(parts_key, part)
    key_hid, key_pick, key_low, key_any, key_pad, key_wt = jax.random.split(part_key, 6)
    key_gain, key_unemb = jax.random.split(shared_key)
    hidden = jax.random.normal(key_hid, (TOKENS, D), jnp.float32).astype(jnp.bfloat16)
    tok_ids = jnp.arange(TOKENS)
    pick_low = jax.random.randint(key_pick, (TOKENS,), 0, 2)
    low_ids = jax.random.randint(key_low, (TOKENS,), 0, LOW_IDS)
    any_ids = jax.random.randint(key_any, (TOKENS,), 0, V)
    labels = jnp.where(pick_low == 0, low_ids, any_ids)
    labels = jnp.where(tok_ids == TOKENS - 1, V - 1, labels).astype(jnp.int32)
    pad_draw = jax.random.randint(key_pad, (TOKENS,), 0, 8)
    is_pad = (pad_draw == 0) & (tok_ids > 0)
    weight_val = jax.random.uniform(key_wt, (TOKENS,), jnp.float32, 0.25, 1.75)
    loss_weight = jnp.where(is_pad, 0.0, weight_val).astype(jnp.float32)
    norm_gain = 1.0 + 0.25 * jax.random.normal(key_gain, (D,), jnp.float32)
    w_unembed = (jax.random.normal(key_unemb, (D, VOCAB_PAD), jnp.float32) * (2.0 * D ** -0.5)).astype(jnp.bfloat16)
    return {"hidden": hidden, "labels": labels, "loss_weight": loss_weight, "norm_gain": norm_gain, "w_unembed": w_unembed}


def reference(hidden, labels, loss_weight, norm_gain, w_unembed):
    x_float = hidden.astype(jnp.float32)
    inv_rms = lax.rsqrt(jnp.mean(x_float * x_float, axis=-1, keepdims=True) + NORM_EPS)
    x_norm = x_float * inv_rms
    normed = (x_norm * norm_gain).astype(jnp.bfloat16)
    tok_scale = loss_weight / jnp.sum(loss_weight)
    col_ids = jnp.arange(VOCAB_PAD)[None, :]

    def block_step(d_unembed, block_in):
        normed_blk, label_blk, scale_blk = block_in
        logits = jnp.dot(normed_blk, w_unembed, preferred_element_type=jnp.float32)
        logits = jnp.where(col_ids < V, logits, -jnp.inf)
        is_target = col_ids == label_blk[:, None]
        row_max = jnp.max(logits, axis=1, keepdims=True)
        log_norm = row_max + jnp.log(jnp.sum(jnp.exp(logits - row_max), axis=1, keepdims=True))
        target = jnp.sum(jnp.where(is_target, logits, 0.0), axis=1, keepdims=True)
        tok_loss = (log_norm - target)[:, 0] * scale_blk
        d_logits = ((jnp.exp(logits - log_norm) - jnp.where(is_target, 1.0, 0.0)) * scale_blk[:, None]).astype(jnp.bfloat16)
        d_unembed = d_unembed + jnp.dot(normed_blk.T, d_logits, preferred_element_type=jnp.float32)
        d_normed = jnp.dot(d_logits, w_unembed.T, preferred_element_type=jnp.float32)
        return d_unembed, (tok_loss, d_normed)

    blocks = (normed.reshape(GROUP_SIZE, TOK_DEV, D), labels.reshape(GROUP_SIZE, TOK_DEV), tok_scale.reshape(GROUP_SIZE, TOK_DEV))
    d_unembed, (tok_loss, d_normed) = lax.scan(block_step, jnp.zeros((D, VOCAB_PAD), jnp.float32), blocks)
    d_normed = d_normed.reshape(TOKENS, D)
    mean_loss = jnp.sum(tok_loss).reshape(1)
    grad_hat = d_normed * norm_gain
    d_input = inv_rms * (grad_hat - x_norm * jnp.mean(grad_hat * x_norm, axis=-1, keepdims=True))
    d_norm_gain = jnp.sum(d_normed * x_norm, axis=0)
    return mean_loss, d_input.astype(jnp.bfloat16), d_unembed, d_norm_gain
```

```python
import functools

import jax
import jax.numpy as jnp
from jax import lax
from jax.experimental import pallas as pl
from jax.experimental.pallas import tpu as pltpu
from jax.sharding import PartitionSpec as P

NORM_EPS = 1e-5
PAD_COLS = 128
LANES = 128
F32 = jnp.float32
BF16 = jnp.bfloat16
LOWEST = float(jnp.finfo(jnp.float32).min)
VMEM_BYTES = 60 * 1024 * 1024
MESH = pl.DeviceIdType.MESH


def slot_block(me, core, step, chips):
    def of(which):
        chip = me // 2
        back = lax.rem(chip + chips - step, chips)
        ahead = lax.rem(chip + step, chips)
        return jnp.where(which == 0, back, ahead) * 2 + which
    return of(core), of(1 - core)


def barrier_all(me, n):
    sem = pltpu.get_barrier_semaphore()
    for d in range(1, n):
        pl.semaphore_signal(sem, inc=1, device_id={"vp": lax.rem(me + d, n)}, device_id_type=MESH)
    pl.semaphore_wait(sem, n - 1)


def share(me, n, send, recv, send_sem, recv_sem):
    copies = []
    for d in range(1, n):
        copy = pltpu.make_async_remote_copy(
            src_ref=send, dst_ref=recv.at[me], send_sem=send_sem.at[d - 1], recv_sem=recv_sem.at[d - 1],
            device_id={"vp": lax.rem(me + d, n)}, device_id_type=MESH)
        copy.start()
        copies.append(copy)
    recv[pl.ds(me, 1)] = send[...][None]
    for copy in copies:
        copy.wait()


def row_tile(count, most):
    return min(range(256, most + 1, 16), key=lambda t: (-(-count // t) * t, -t))


def logits_kernel(lim_ref, h_ref, p_ref, w_ref, z_ref, st_ref, max_s, sum_s, *, parts):
    j = pl.program_id(0)
    tile = w_ref.shape[0]
    limit = lim_ref[0]

    @pl.when(j == 0)
    def _():
        max_s[...] = jnp.full(max_s.shape, LOWEST, F32)
        sum_s[...] = jnp.zeros(sum_s.shape, F32)

    a = jnp.concatenate([h_ref[...], p_ref[...]], axis=0)
    row0 = 0
    for part in parts:
        z = lax.dot_general(w_ref[row0:row0 + part, :], a, (((1,), (1,)), ((), ())), preferred_element_type=F32)
        row = lax.broadcasted_iota(jnp.int32, z.shape, 0) + (j * tile + row0)
        z = jnp.where(row < limit, z, -jnp.inf)
        z_ref[row0:row0 + part, :] = z
        z = z.reshape(part // 8, 8, z.shape[1])
        old = max_s[...]
        new = jnp.maximum(old, jnp.max(z, axis=0))
        max_s[...] = new
        sum_s[...] = sum_s[...] * jnp.exp(old - new) + jnp.sum(jnp.exp(z - new[None]), axis=0)
        row0 += part

    @pl.when(j == pl.num_programs(0) - 1)
    def _():
        top = jnp.max(max_s[...], axis=0, keepdims=True)
        total = jnp.sum(sum_s[...] * jnp.exp(max_s[...] - top), axis=0, keepdims=True)
        st_ref[...] = jnp.where(lax.broadcasted_iota(jnp.int32, st_ref.shape, 0) == 0, top, total)


def logits_call(limit, h, p, wt, most=704, tile=None, parts=None):
    rows, depth = h.shape
    cols = wt.shape[0]
    tile = tile or row_tile(cols, most)
    first = tile // 32 * 16
    parts = parts or (tile - first, first)
    return pl.pallas_call(
        functools.partial(logits_kernel, parts=parts),
        grid=(-(-cols // tile),),
        in_specs=[
            pl.BlockSpec(memory_space=pltpu.SMEM),
            pl.BlockSpec((rows, depth), lambda j: (0, 0)),
            pl.BlockSpec((rows, depth), lambda j: (0, 0)),
            pl.BlockSpec((tile, depth), lambda j: (j, 0)),
        ],
        out_specs=[
            pl.BlockSpec((tile, 2 * rows), lambda j: (j, 0)),
            pl.BlockSpec((8, 2 * rows), lambda j: (0, 0)),
        ],
        out_shape=[
            jax.ShapeDtypeStruct((cols, 2 * rows), F32),
            jax.ShapeDtypeStruct((8, 2 * rows), F32),
        ],
        scratch_shapes=[pltpu.VMEM((8, 2 * rows), F32)] * 2,
        compiler_params=pltpu.CompilerParams(vmem_limit_bytes=VMEM_BYTES),
        cost_estimate=pl.CostEstimate(
            flops=2 * 2 * rows * depth * cols, bytes_accessed=depth * cols * 2 + 2 * rows * cols * 4,
            transcendentals=2 * rows * cols),
        name="logits",
    )(limit, h, p, wt)


def stats_kernel(n, *refs):
    chips = n // 2
    st_refs = refs[:chips]
    lw_ref = refs[chips]
    out_refs = refs[chips + 1:2 * chips + 1]
    loss_ref, send, recv, table, send_sem, recv_sem = refs[2 * chips + 1:]
    me = lax.axis_index("vp")
    core = lax.rem(me, 2)
    rows = lw_ref.shape[1]
    for step in range(chips):
        for half, block in enumerate(slot_block(me, core, step, chips)):
            span = pl.ds(half * rows, rows)
            send[pl.ds(block, 1), :] = st_refs[step][0:1, span]
            send[pl.ds(n + block, 1), :] = st_refs[step][1:2, span]
    send[2 * n:2 * n + 8, :] = lw_ref[...]
    barrier_all(me, n)
    share(me, n, send, recv, send_sem, recv_sem)
    top = recv[0, 0:n, :]
    for i in range(1, n):
        top = jnp.maximum(top, recv[i, 0:n, :])
    total = jnp.zeros_like(top)
    for i in range(n):
        total = total + recv[i, n:2 * n, :] * jnp.exp(recv[i, 0:n, :] - top)
    log_norm = top + jnp.log(total)
    labels = jnp.concatenate([recv[i, 2 * n:2 * n + 1, :] for i in range(n)], axis=0)
    weights = jnp.concatenate([recv[i, 2 * n + 1:2 * n + 2, :] for i in range(n)], axis=0)
    scale = weights / jnp.sum(jnp.sum(weights, axis=1, keepdims=True), axis=0, keepdims=True)
    loss = jnp.sum(jnp.sum(scale * log_norm, axis=1, keepdims=True), axis=0, keepdims=True)
    loss_ref[...] = jnp.broadcast_to(loss, loss_ref.shape)
    table[0:n, :] = log_norm
    table[n:2 * n, :] = scale
    table[2 * n:3 * n, :] = labels
    for step in range(chips):
        for half, block in enumerate(slot_block(me, core, step, chips)):
            for k in range(3):
                out_refs[step][k:k + 1, half * rows:(half + 1) * rows] = table[pl.ds(k * n + block, 1), :]


def stats_call(stats, label_weight, n):
    rows = label_weight.shape[1]
    vmem = pl.BlockSpec(memory_space=pltpu.VMEM)
    return pl.pallas_call(
        functools.partial(stats_kernel, n),
        in_specs=[vmem] * (len(stats) + 1),
        out_specs=[vmem] * (len(stats) + 1),
        out_shape=[jax.ShapeDtypeStruct((8, 2 * rows), F32)] * len(stats) + [jax.ShapeDtypeStruct((8, LANES), F32)],
        scratch_shapes=[
            pltpu.VMEM((2 * n + 8, rows), F32),
            pltpu.VMEM((n, 2 * n + 8, rows), F32),
            pltpu.VMEM((3 * n, rows), F32),
            pltpu.SemaphoreType.DMA((n - 1,)),
            pltpu.SemaphoreType.DMA((n - 1,)),
        ],
        compiler_params=pltpu.CompilerParams(collective_id=1, has_side_effects=True),
        cost_estimate=pl.CostEstimate(flops=4_000_000_000, bytes_accessed=n * rows * 512, transcendentals=0),
        name="stats",
    )(*stats, label_weight)


def total_kernel(n, x_ref, out_ref, recv, send_sem, recv_sem):
    me = lax.axis_index("vp")
    barrier_all(me, n)
    share(me, n, x_ref, recv, send_sem, recv_sem)
    total = recv[0]
    for i in range(1, n):
        total = total + recv[i]
    out_ref[...] = total


def total_call(x, n):
    vmem = pl.BlockSpec(memory_space=pltpu.VMEM)
    return pl.pallas_call(
        functools.partial(total_kernel, n),
        in_specs=[vmem],
        out_specs=vmem,
        out_shape=jax.ShapeDtypeStruct(x.shape, F32),
        scratch_shapes=[
            pltpu.VMEM((n,) + x.shape, F32), pltpu.SemaphoreType.DMA((n - 1,)), pltpu.SemaphoreType.DMA((n - 1,))],
        compiler_params=pltpu.CompilerParams(collective_id=2, has_side_effects=True),
        cost_estimate=pl.CostEstimate(flops=4_000_000_000, bytes_accessed=x.size * 4 * n, transcendentals=0),
        name="total",
    )(x)


def g_kernel(first_ref, row_ref, z_ref, w_ref, dzt_ref, gh_ref, gp_ref, hit_ref, *, cols, parts):
    j = pl.program_id(0)
    tile, tokens = z_ref.shape
    rows = tokens // 2
    last = pl.num_programs(0) - 1
    log_norm, scale = row_ref[0:1, :], row_ref[1:2, :]
    label = row_ref[2:3, :].astype(jnp.int32) - first_ref[0]
    label = jnp.where(label < cols, label, -1) - j * tile

    @pl.when(j == 0)
    def _():
        hit_ref[...] = jnp.zeros_like(hit_ref)
        gh_ref[...] = jnp.zeros_like(gh_ref)
        gp_ref[...] = jnp.zeros_like(gp_ref)

    def block(row0, count):
        z = z_ref[row0:row0 + count, :]
        is_target = lax.broadcasted_iota(jnp.int32, z.shape, 0) + row0 == label
        d = ((jnp.exp(z - log_norm) - jnp.where(is_target, 1.0, 0.0)) * scale).astype(BF16)
        dzt_ref[row0:row0 + count, :] = d
        hit_ref[...] += jnp.sum(jnp.where(is_target, z, 0.0).reshape(count // 8, 8, tokens), axis=0) * scale
        g = lax.dot_general(d, w_ref[row0:row0 + count, :], (((0,), (0,)), ((), ())), preferred_element_type=F32)
        gh_ref[...] += g[:rows]
        gp_ref[...] += g[rows:]

    rest = cols % tile
    if rest:
        @pl.when(j < last)
        def _():
            for k in range(parts):
                block(k * (tile // parts), tile // parts)

        @pl.when(j == last)
        def _():
            block(0, rest)
    else:
        for k in range(parts):
            block(k * (tile // parts), tile // parts)


def g_call(first_col, table, z, wt, tile=512, parts=2):
    cols, tokens = z.shape
    depth = wt.shape[1]
    whole = pl.BlockSpec((tokens // 2, depth), lambda j: (0, 0))
    shape = jax.ShapeDtypeStruct((tokens // 2, depth), F32)
    return pl.pallas_call(
        functools.partial(g_kernel, cols=cols, parts=parts),
        grid=(-(-cols // tile),),
        in_specs=[
            pl.BlockSpec(memory_space=pltpu.SMEM),
            pl.BlockSpec((8, tokens), lambda j: (0, 0)),
            pl.BlockSpec((tile, tokens), lambda j: (j, 0)),
            pl.BlockSpec((tile, depth), lambda j: (j, 0)),
        ],
        out_specs=[pl.BlockSpec((tile, tokens), lambda j: (j, 0)), whole, whole, pl.BlockSpec((8, tokens), lambda j: (0, 0))],
        out_shape=[jax.ShapeDtypeStruct((cols, tokens), BF16), shape, shape, jax.ShapeDtypeStruct((8, tokens), F32)],
        compiler_params=pltpu.CompilerParams(vmem_limit_bytes=VMEM_BYTES),
        cost_estimate=pl.CostEstimate(
            flops=2 * tokens * cols * depth, bytes_accessed=depth * cols * 2 + tokens * depth * 4 + tokens * cols * 6,
            transcendentals=tokens * cols),
        name="gmm",
    )(first_col, table, z, wt)


def dw_kernel(*refs, blocks, chunks):
    out_ref = refs[-1]
    a = jnp.concatenate([r[...] for r in refs[:blocks]], axis=0)
    dz = jnp.concatenate([r[...] for r in refs[blocks:blocks + chunks]], axis=1)
    out_ref[...] = jnp.dot(dz, a, preferred_element_type=F32)


def dw_call(a_blocks, dz_chunks, start, count, previous=None, wide=1024, most=704):
    rows, depth = a_blocks[0].shape
    cols, chunk = dz_chunks[0].shape
    tile = row_tile(cols, most)
    base = start // wide
    specs = [pl.BlockSpec((rows, wide), lambda i, j: (0, i + base))] * len(a_blocks)
    specs += [pl.BlockSpec((tile, chunk), lambda i, j: (j, 0))] * len(dz_chunks)
    args = list(a_blocks) + list(dz_chunks)
    aliases = {}
    if previous is not None:
        aliases = {len(args): 0}
        specs.append(pl.BlockSpec(memory_space=pl.ANY))
        args.append(previous)
    tokens = chunk * len(dz_chunks)
    return pl.pallas_call(
        functools.partial(dw_kernel, blocks=len(a_blocks), chunks=len(dz_chunks)),
        grid=(count // wide, -(-cols // tile)),
        in_specs=specs,
        out_specs=pl.BlockSpec((tile, wide), lambda i, j: (j, i + base)),
        out_shape=jax.ShapeDtypeStruct((cols, depth), F32),
        input_output_aliases=aliases,
        compiler_params=pltpu.CompilerParams(vmem_limit_bytes=VMEM_BYTES),
        cost_estimate=pl.CostEstimate(
            flops=2 * tokens * count * cols, bytes_accessed=count * cols * 4 + tokens * cols * 2, transcendentals=0),
        name="dunembed",
    )(*args)


def solution(mesh):
    n = mesh.shape["vp"]
    chips = n // 2
    swap = [(i, i ^ 1) for i in range(n)]
    ring = []
    for i in range(n):
        chip, core = i // 2, i % 2
        ring.append((i, ((chip + 1 if core == 0 else chip - 1) % chips) * 2 + core))

    def send(x, to):
        return lax.ppermute(x, "vp", to)

    def after(x, y):
        return lax.optimization_barrier((x, y))[0]

    def local_step(hidden, labels, loss_weight, norm_gain, w_local):
        rows, depth = hidden.shape
        cols = w_local.shape[1]
        wt = w_local.T
        first = lax.axis_index("vp") * cols
        limit = jnp.minimum(cols, cols * n - PAD_COLS - first).reshape(1)
        x_float = hidden.astype(F32)
        inv_rms = lax.rsqrt(jnp.mean(x_float * x_float, axis=-1, keepdims=True) + NORM_EPS)
        x_norm = x_float * inv_rms
        own = [(x_norm * norm_gain).astype(BF16)]
        partner = []
        logits = []
        for s in range(chips):
            partner.append(send(own[s], swap))
            if s < chips - 1:
                arriving = send(own[s], ring)
            logits.append(logits_call(limit, own[s], partner[s], wt))
            if s < chips - 1:
                own.append(after(arriving, logits[s][1]))
        label_weight = jnp.zeros((8, rows), F32).at[0].set(labels.astype(F32)).at[1].set(loss_weight)
        *tables, loss_a = stats_call([x[1] for x in logits], label_weight, n)
        order = list(range(1, chips)) + [0]
        dz_t, hits, grads = {}, [], {}
        for s in order:
            dz_t[s], own_part, other_part, hit = g_call(first.reshape(1), tables[s], logits[s][0], wt)
            hits.append(hit)
            grads[s] = (own_part, send(other_part, swap))
        a_blocks = [x for s in range(chips) for x in (own[s], partner[s])]
        dzs = [dz_t[s] for s in range(chips)]
        half = depth // 2
        moving = None
        for i, s in enumerate(order):
            acc = grads[s][0] + grads[s][1]
            if moving is not None:
                acc = acc + moving
            if s != 0:
                moving = send(acc, ring)
            if i == 0:
                moving = after(moving, hits[-1])
            if i == chips - 3:
                d_unembed = dw_call(a_blocks, dzs, 0, half)
                moving, d_unembed = lax.optimization_barrier((moving, d_unembed))
            if i == chips - 2:
                d_unembed = dw_call(a_blocks, dzs, half, half, d_unembed)
                moving, d_unembed = lax.optimization_barrier((moving, d_unembed))
        d_unembed = d_unembed.T
        d_normed = acc
        grad_hat = d_normed * norm_gain
        d_input = inv_rms * (grad_hat - x_norm * jnp.mean(grad_hat * x_norm, axis=-1, keepdims=True))
        part = jnp.sum(d_normed * x_norm, axis=0).reshape(depth // LANES, LANES)
        hit = functools.reduce(jnp.add, hits)
        total = total_call(jnp.concatenate([part, hit.reshape(-1, LANES)], axis=0), n)
        d_norm_gain = total[:depth // LANES].reshape(depth)
        mean_loss = (loss_a[0, 0] - jnp.sum(total[depth // LANES:])).reshape(1)
        return mean_loss, d_input.astype(BF16), d_unembed, d_norm_gain

    return jax.shard_map(
        local_step,
        mesh=mesh,
        in_specs=(P(("dp", "vp"), None), P(("dp", "vp")), P(("dp", "vp")), P(None), P(None, "vp")),
        out_specs=(P("dp"), P(("dp", "vp"), None), P("dp", "vp"), P("dp")),
        check_vma=False,
    )
```

```python
import functools

import jax
import jax.numpy as jnp
from jax import lax
from jax.experimental import pallas as pl
from jax.experimental.pallas import tpu as pltpu
from jax.sharding import PartitionSpec as P

NORM_EPS = 1e-5
PAD_COLS = 128
LANES = 128
F32 = jnp.float32
BF16 = jnp.bfloat16
LOWEST = float(jnp.finfo(jnp.float32).min)
VMEM_BYTES = 60 * 1024 * 1024
MESH = pl.DeviceIdType.MESH


def slot_block(me, core, step, chips):
    def of(which):
        chip = me // 2
        back = lax.rem(chip + chips - step, chips)
        ahead = lax.rem(chip + step, chips)
        return jnp.where(which == 0, back, ahead) * 2 + which
    return of(core), of(1 - core)


def barrier_all(me, n):
    sem = pltpu.get_barrier_semaphore()
    for d in range(1, n):
        pl.semaphore_signal(sem, inc=1, device_id={"vp": lax.rem(me + d, n)}, device_id_type=MESH)
    pl.semaphore_wait(sem, n - 1)


def share(me, n, send, recv, send_sem, recv_sem):
    copies = []
    for d in range(1, n):
        copy = pltpu.make_async_remote_copy(
            src_ref=send, dst_ref=recv.at[me], send_sem=send_sem.at[d - 1], recv_sem=recv_sem.at[d - 1],
            device_id={"vp": lax.rem(me + d, n)}, device_id_type=MESH)
        copy.start()
        copies.append(copy)
    recv[pl.ds(me, 1)] = send[...][None]
    for copy in copies:
        copy.wait()


def row_tile(count, most):
    return min(range(256, most + 1, 16), key=lambda t: (-(-count // t) * t, -t))


def logits_kernel(lim_ref, x_ref, w_ref, z_ref, st_ref, all_ref, held, max_s, sum_s,
                  next_send, next_recv, swap_send, swap_recv, in_sem, out_sem, *, n, parts):
    chips = n // 2
    s, j = pl.program_id(0), pl.program_id(1)
    steps = pl.num_programs(1)
    tile = w_ref.shape[0]
    rows, depth = x_ref.shape
    half = rows // 2
    me = lax.axis_index("vp")
    chip, core = me // 2, lax.rem(me, 2)
    ahead, back = lax.rem(chip + 1, chips), lax.rem(chip + chips - 1, chips)
    to = jnp.where(core == 0, ahead, back) * 2 + core
    frm = jnp.where(core == 0, back, ahead) * 2 + core
    mate = chip * 2 + 1 - core

    def part_of(k, b):
        return (x_ref if k == 0 else held.at[2 * k]).at[pl.ds(b * half, half)]

    def hop(k, b):
        return pltpu.make_async_remote_copy(
            src_ref=part_of(k, b), dst_ref=held.at[2 * k + 2, pl.ds(b * half, half)],
            send_sem=next_send.at[k, b], recv_sem=next_recv.at[k, b], device_id={"vp": to}, device_id_type=MESH)

    def swap(k, b):
        return pltpu.make_async_remote_copy(
            src_ref=part_of(k, b), dst_ref=held.at[2 * k + 1, pl.ds(b * half, half)],
            send_sem=swap_send.at[k, b], recv_sem=swap_recv.at[k, b], device_id={"vp": mate}, device_id_type=MESH)

    def keep(k):
        return pltpu.make_async_copy(held.at[k], all_ref.at[k], out_sem.at[k])

    @pl.when((s == 0) & (j == 0))
    def _():
        sem = pltpu.get_barrier_semaphore()
        for peer in (to, frm, mate):
            pl.semaphore_signal(sem, inc=1, device_id={"vp": peer}, device_id_type=MESH)
        pl.semaphore_wait(sem, 3)
        own = pltpu.make_async_copy(x_ref, held.at[0], in_sem)
        own.start()
        for b in range(2):
            swap(0, b).start()
            hop(0, b).start()
        own.wait()

    for k in range(chips):
        @pl.when((s == k) & (j == 0))
        def _():
            for b in range(2):
                swap(k, b).wait_recv()
            keep(2 * k).start()
            keep(2 * k + 1).start()

        if k < chips - 1:
            for b, when in ((0, steps // 2), (1, steps - 1)):
                @pl.when((s == k) & (j == when))
                def _():
                    hop(k, b).wait_recv()
                    if k < chips - 2:
                        hop(k + 1, b).start()
                    swap(k + 1, b).start()

    @pl.when(j == 0)
    def _():
        max_s[...] = jnp.full(max_s.shape, LOWEST, F32)
        sum_s[...] = jnp.zeros(sum_s.shape, F32)

    limit = lim_ref[0]
    a = held[pl.ds(2 * s, 2)].reshape(2 * rows, depth)
    row0 = 0
    for part in parts:
        z = lax.dot_general(w_ref[row0:row0 + part, :], a, (((1,), (1,)), ((), ())), preferred_element_type=F32)
        row = lax.broadcasted_iota(jnp.int32, z.shape, 0) + (j * tile + row0)
        z = jnp.where(row < limit, z, -jnp.inf)
        z_ref[row0:row0 + part, :] = z
        z = z.reshape(part // 8, 8, z.shape[1])
        old = max_s[...]
        new = jnp.maximum(old, jnp.max(z, axis=0))
        max_s[...] = new
        sum_s[...] = sum_s[...] * jnp.exp(old - new) + jnp.sum(jnp.exp(z - new[None]), axis=0)
        row0 += part

    @pl.when(j == steps - 1)
    def _():
        top = jnp.max(max_s[...], axis=0, keepdims=True)
        total = jnp.sum(sum_s[...] * jnp.exp(max_s[...] - top), axis=0, keepdims=True)
        st_ref[...] = jnp.where(lax.broadcasted_iota(jnp.int32, st_ref.shape, 0) == 0, top, total)

    @pl.when((s == chips - 1) & (j == steps - 1))
    def _():
        for k in range(chips):
            for b in range(2):
                if k < chips - 1:
                    hop(k, b).wait_send()
                swap(k, b).wait_send()
            keep(2 * k).wait()
            keep(2 * k + 1).wait()


def logits_call(limit, normed, wt, n, most=704):
    rows, depth = normed.shape
    chips = n // 2
    cols = wt.shape[0]
    tile = row_tile(cols, most)
    first = tile // 32 * 16
    sems = pltpu.SemaphoreType.DMA
    return pl.pallas_call(
        functools.partial(logits_kernel, n=n, parts=(tile - first, first)),
        grid=(chips, -(-cols // tile)),
        in_specs=[
            pl.BlockSpec(memory_space=pltpu.SMEM),
            pl.BlockSpec(memory_space=pl.ANY),
            pl.BlockSpec((tile, depth), lambda s, j: (j, 0)),
        ],
        out_specs=[
            pl.BlockSpec((None, tile, 2 * rows), lambda s, j: (s, j, 0)),
            pl.BlockSpec((None, 8, 2 * rows), lambda s, j: (s, 0, 0)),
            pl.BlockSpec(memory_space=pl.ANY),
        ],
        out_shape=[
            jax.ShapeDtypeStruct((chips, cols, 2 * rows), F32),
            jax.ShapeDtypeStruct((chips, 8, 2 * rows), F32),
            jax.ShapeDtypeStruct((n, rows, depth), BF16),
        ],
        scratch_shapes=[
            pltpu.VMEM((n, rows, depth), BF16),
            pltpu.VMEM((8, 2 * rows), F32),
            pltpu.VMEM((8, 2 * rows), F32),
            sems((chips - 1, 2)), sems((chips - 1, 2)), sems((chips, 2)), sems((chips, 2)), sems, sems((n,)),
        ],
        compiler_params=pltpu.CompilerParams(vmem_limit_bytes=VMEM_BYTES, collective_id=0, has_side_effects=True),
        cost_estimate=pl.CostEstimate(
            flops=2 * n * rows * depth * cols, bytes_accessed=chips * depth * cols * 2 + n * rows * cols * 4,
            transcendentals=n * rows * cols),
        name="logits",
    )(limit, normed, wt)


def stats_kernel(n, *refs):
    chips = n // 2
    st_ref, lw_ref = refs[:2]
    out_refs = refs[2:chips + 2]
    loss_ref, send, recv, table, send_sem, recv_sem = refs[chips + 2:]
    me = lax.axis_index("vp")
    core = lax.rem(me, 2)
    rows = lw_ref.shape[1]
    for step in range(chips):
        for half, block in enumerate(slot_block(me, core, step, chips)):
            span = pl.ds(half * rows, rows)
            send[pl.ds(block, 1), :] = st_ref[step, 0:1, span]
            send[pl.ds(n + block, 1), :] = st_ref[step, 1:2, span]
    send[2 * n:2 * n + 8, :] = lw_ref[...]
    barrier_all(me, n)
    share(me, n, send, recv, send_sem, recv_sem)
    top = recv[0, 0:n, :]
    for i in range(1, n):
        top = jnp.maximum(top, recv[i, 0:n, :])
    total = jnp.zeros_like(top)
    for i in range(n):
        total = total + recv[i, n:2 * n, :] * jnp.exp(recv[i, 0:n, :] - top)
    log_norm = top + jnp.log(total)
    labels = jnp.concatenate([recv[i, 2 * n:2 * n + 1, :] for i in range(n)], axis=0)
    weights = jnp.concatenate([recv[i, 2 * n + 1:2 * n + 2, :] for i in range(n)], axis=0)
    scale = weights / jnp.sum(jnp.sum(weights, axis=1, keepdims=True), axis=0, keepdims=True)
    loss = jnp.sum(jnp.sum(scale * log_norm, axis=1, keepdims=True), axis=0, keepdims=True)
    loss_ref[...] = jnp.broadcast_to(loss, loss_ref.shape)
    table[0:n, :] = log_norm
    table[n:2 * n, :] = scale
    table[2 * n:3 * n, :] = labels
    for step in range(chips):
        for half, block in enumerate(slot_block(me, core, step, chips)):
            for k in range(3):
                out_refs[step][k:k + 1, half * rows:(half + 1) * rows] = table[pl.ds(k * n + block, 1), :]


def stats_call(stats, label_weight, n):
    rows = label_weight.shape[1]
    vmem = pl.BlockSpec(memory_space=pltpu.VMEM)
    return pl.pallas_call(
        functools.partial(stats_kernel, n),
        in_specs=[vmem, vmem],
        out_specs=[vmem] * (n // 2 + 1),
        out_shape=[jax.ShapeDtypeStruct((8, 2 * rows), F32)] * (n // 2) + [jax.ShapeDtypeStruct((8, LANES), F32)],
        scratch_shapes=[
            pltpu.VMEM((2 * n + 8, rows), F32),
            pltpu.VMEM((n, 2 * n + 8, rows), F32),
            pltpu.VMEM((3 * n, rows), F32),
            pltpu.SemaphoreType.DMA((n - 1,)),
            pltpu.SemaphoreType.DMA((n - 1,)),
        ],
        compiler_params=pltpu.CompilerParams(collective_id=1, has_side_effects=True),
        cost_estimate=pl.CostEstimate(flops=4_000_000_000, bytes_accessed=n * rows * 512, transcendentals=0),
        name="stats",
    )(stats, label_weight)


def total_kernel(n, x_ref, out_ref, recv, send_sem, recv_sem):
    me = lax.axis_index("vp")
    barrier_all(me, n)
    share(me, n, x_ref, recv, send_sem, recv_sem)
    total = recv[0]
    for i in range(1, n):
        total = total + recv[i]
    out_ref[...] = total


def total_call(x, n):
    vmem = pl.BlockSpec(memory_space=pltpu.VMEM)
    return pl.pallas_call(
        functools.partial(total_kernel, n),
        in_specs=[vmem],
        out_specs=vmem,
        out_shape=jax.ShapeDtypeStruct(x.shape, F32),
        scratch_shapes=[
            pltpu.VMEM((n,) + x.shape, F32), pltpu.SemaphoreType.DMA((n - 1,)), pltpu.SemaphoreType.DMA((n - 1,))],
        compiler_params=pltpu.CompilerParams(collective_id=2, has_side_effects=True),
        cost_estimate=pl.CostEstimate(flops=4_000_000_000, bytes_accessed=x.size * 4 * n, transcendentals=0),
        name="total",
    )(x)


def g_kernel(first_ref, row_ref, z_ref, w_ref, dzt_ref, gh_ref, gp_ref, hit_ref, *, cols, parts):
    j = pl.program_id(0)
    tile, tokens = z_ref.shape
    rows = tokens // 2
    last = pl.num_programs(0) - 1
    log_norm, scale = row_ref[0:1, :], row_ref[1:2, :]
    label = row_ref[2:3, :].astype(jnp.int32) - first_ref[0]
    label = jnp.where(label < cols, label, -1) - j * tile

    @pl.when(j == 0)
    def _():
        hit_ref[...] = jnp.zeros_like(hit_ref)
        gh_ref[...] = jnp.zeros_like(gh_ref)
        gp_ref[...] = jnp.zeros_like(gp_ref)

    def block(row0, count):
        z = z_ref[row0:row0 + count, :]
        is_target = lax.broadcasted_iota(jnp.int32, z.shape, 0) + row0 == label
        d = ((jnp.exp(z - log_norm) - jnp.where(is_target, 1.0, 0.0)) * scale).astype(BF16)
        dzt_ref[row0:row0 + count, :] = d
        hit_ref[...] += jnp.sum(jnp.where(is_target, z, 0.0).reshape(count // 8, 8, tokens), axis=0) * scale
        g = lax.dot_general(d, w_ref[row0:row0 + count, :], (((0,), (0,)), ((), ())), preferred_element_type=F32)
        gh_ref[...] += g[:rows]
        gp_ref[...] += g[rows:]

    rest = cols % tile
    if rest:
        @pl.when(j < last)
        def _():
            for k in range(parts):
                block(k * (tile // parts), tile // parts)

        @pl.when(j == last)
        def _():
            block(0, rest)
    else:
        for k in range(parts):
            block(k * (tile // parts), tile // parts)


def g_call(first_col, table, z, slot, wt, tile=512, parts=2):
    cols, tokens = z.shape[1:]
    depth = wt.shape[1]
    whole = pl.BlockSpec((tokens // 2, depth), lambda j: (0, 0))
    shape = jax.ShapeDtypeStruct((tokens // 2, depth), F32)
    return pl.pallas_call(
        functools.partial(g_kernel, cols=cols, parts=parts),
        grid=(-(-cols // tile),),
        in_specs=[
            pl.BlockSpec(memory_space=pltpu.SMEM),
            pl.BlockSpec((8, tokens), lambda j: (0, 0)),
            pl.BlockSpec((None, tile, tokens), lambda j: (slot, j, 0)),
            pl.BlockSpec((tile, depth), lambda j: (j, 0)),
        ],
        out_specs=[pl.BlockSpec((tile, tokens), lambda j: (j, 0)), whole, whole, pl.BlockSpec((8, tokens), lambda j: (0, 0))],
        out_shape=[jax.ShapeDtypeStruct((cols, tokens), BF16), shape, shape, jax.ShapeDtypeStruct((8, tokens), F32)],
        compiler_params=pltpu.CompilerParams(vmem_limit_bytes=VMEM_BYTES),
        cost_estimate=pl.CostEstimate(
            flops=2 * tokens * cols * depth, bytes_accessed=depth * cols * 2 + tokens * depth * 4 + tokens * cols * 6,
            transcendentals=tokens * cols),
        name="gmm",
    )(first_col, table, z, wt)


def dw_kernel(a_ref, *refs, chunks):
    out_ref = refs[-1]
    a = a_ref[...].reshape(-1, a_ref.shape[-1])
    dz = jnp.concatenate([r[...] for r in refs[:chunks]], axis=1)
    out_ref[...] = jnp.dot(dz, a, preferred_element_type=F32)


def dw_call(a, dz_chunks, start, count, previous=None, wide=1024, most=704):
    n, rows, depth = a.shape
    cols, chunk = dz_chunks[0].shape
    tile = row_tile(cols, most)
    base = start // wide
    specs = [pl.BlockSpec((n, rows, wide), lambda i, j: (0, 0, i + base))]
    specs += [pl.BlockSpec((tile, chunk), lambda i, j: (j, 0))] * len(dz_chunks)
    args = [a] + list(dz_chunks)
    aliases = {}
    if previous is not None:
        aliases = {len(args): 0}
        specs.append(pl.BlockSpec(memory_space=pl.ANY))
        args.append(previous)
    tokens = chunk * len(dz_chunks)
    return pl.pallas_call(
        functools.partial(dw_kernel, chunks=len(dz_chunks)),
        grid=(count // wide, -(-cols // tile)),
        in_specs=specs,
        out_specs=pl.BlockSpec((tile, wide), lambda i, j: (j, i + base)),
        out_shape=jax.ShapeDtypeStruct((cols, depth), F32),
        input_output_aliases=aliases,
        compiler_params=pltpu.CompilerParams(vmem_limit_bytes=VMEM_BYTES),
        cost_estimate=pl.CostEstimate(
            flops=2 * tokens * count * cols, bytes_accessed=count * cols * 4 + tokens * cols * 2, transcendentals=0),
        name="dunembed",
    )(*args)


def solution(mesh):
    n = mesh.shape["vp"]
    chips = n // 2
    swap = [(i, i ^ 1) for i in range(n)]
    ring = []
    for i in range(n):
        chip, core = i // 2, i % 2
        ring.append((i, ((chip + 1 if core == 0 else chip - 1) % chips) * 2 + core))

    def send(x, to):
        return lax.ppermute(x, "vp", to)

    def after(x, y):
        return lax.optimization_barrier((x, y))[0]

    def local_step(hidden, labels, loss_weight, norm_gain, w_local):
        rows, depth = hidden.shape
        cols = w_local.shape[1]
        wt = w_local.T
        first = lax.axis_index("vp") * cols
        limit = jnp.minimum(cols, cols * n - PAD_COLS - first).reshape(1)
        x_float = hidden.astype(F32)
        inv_rms = lax.rsqrt(jnp.mean(x_float * x_float, axis=-1, keepdims=True) + NORM_EPS)
        x_norm = x_float * inv_rms
        normed = (x_norm * norm_gain).astype(BF16)
        logits, stats, a_all = logits_call(limit, normed, wt, n)
        label_weight = jnp.zeros((8, rows), F32).at[0].set(labels.astype(F32)).at[1].set(loss_weight)
        *tables, loss_a = stats_call(stats, label_weight, n)
        order = list(range(1, chips)) + [0]
        dz_t, hits, grads = {}, [], {}
        for s in order:
            dz_t[s], own_part, other_part, hit = g_call(first.reshape(1), tables[s], logits, s, wt)
            hits.append(hit)
            grads[s] = (own_part, send(other_part, swap))
        dzs = [dz_t[s] for s in range(chips)]
        half = depth // 2
        moving = None
        for i, s in enumerate(order):
            acc = grads[s][0] + grads[s][1]
            if moving is not None:
                acc = acc + moving
            if s != 0:
                moving = send(acc, ring)
            if i == 0:
                moving = after(moving, hits[-1])
            if i == chips - 3:
                d_unembed = dw_call(a_all, dzs, 0, half)
                moving, d_unembed = lax.optimization_barrier((moving, d_unembed))
            if i == chips - 2:
                d_unembed = dw_call(a_all, dzs, half, half, d_unembed)
                moving, d_unembed = lax.optimization_barrier((moving, d_unembed))
        d_unembed = d_unembed.T
        d_normed = acc
        grad_hat = d_normed * norm_gain
        d_input = inv_rms * (grad_hat - x_norm * jnp.mean(grad_hat * x_norm, axis=-1, keepdims=True))
        part = jnp.sum(d_normed * x_norm, axis=0).reshape(depth // LANES, LANES)
        hit = functools.reduce(jnp.add, hits)
        total = total_call(jnp.concatenate([part, hit.reshape(-1, LANES)], axis=0), n)
        d_norm_gain = total[:depth // LANES].reshape(depth)
        mean_loss = (loss_a[0, 0] - jnp.sum(total[depth // LANES:])).reshape(1)
        return mean_loss, d_input.astype(BF16), d_unembed, d_norm_gain

    return jax.shard_map(
        local_step,
        mesh=mesh,
        in_specs=(P(("dp", "vp"), None), P(("dp", "vp")), P(("dp", "vp")), P(None), P(None, "vp")),
        out_specs=(P("dp"), P(("dp", "vp"), None), P("dp", "vp"), P("dp")),
        check_vma=False,
    )
```

```python
import functools

import jax
import jax.numpy as jnp
from jax import lax
from jax.experimental import pallas as pl
from jax.experimental.pallas import tpu as pltpu
from jax.sharding import PartitionSpec as P

NORM_EPS = 1e-5
PAD_COLS = 128
LANES = 128
F32 = jnp.float32
BF16 = jnp.bfloat16
LOWEST = float(jnp.finfo(jnp.float32).min)
VMEM_BYTES = 60 * 1024 * 1024
MESH = pl.DeviceIdType.MESH


def slot_block(me, core, step, chips):
    def of(which):
        chip = me // 2
        back = lax.rem(chip + chips - step, chips)
        ahead = lax.rem(chip + step, chips)
        return jnp.where(which == 0, back, ahead) * 2 + which
    return of(core), of(1 - core)


def barrier_all(me, n):
    sem = pltpu.get_barrier_semaphore()
    for d in range(1, n):
        pl.semaphore_signal(sem, inc=1, device_id={"vp": lax.rem(me + d, n)}, device_id_type=MESH)
    pl.semaphore_wait(sem, n - 1)


def share(me, n, send, recv, send_sem, recv_sem):
    copies = []
    for d in range(1, n):
        copy = pltpu.make_async_remote_copy(
            src_ref=send, dst_ref=recv.at[me], send_sem=send_sem.at[d - 1], recv_sem=recv_sem.at[d - 1],
            device_id={"vp": lax.rem(me + d, n)}, device_id_type=MESH)
        copy.start()
        copies.append(copy)
    recv[pl.ds(me, 1)] = send[...][None]
    for copy in copies:
        copy.wait()


def row_tile(count, most):
    return min(range(256, most + 1, 16), key=lambda t: (-(-count // t) * t, -t))


def logits_kernel(lim_ref, x_ref, w_ref, z_ref, st_ref, all_ref, held, max_s, sum_s, tail_s,
                  next_send, next_recv, swap_send, swap_recv, in_sem, out_sem, *, n, parts):
    chips = n // 2
    s, j = pl.program_id(0), pl.program_id(1)
    steps = pl.num_programs(1)
    tile = w_ref.shape[0]
    rows, depth = x_ref.shape
    half = rows // 2
    me = lax.axis_index("vp")
    chip, core = me // 2, lax.rem(me, 2)
    ahead, back = lax.rem(chip + 1, chips), lax.rem(chip + chips - 1, chips)
    to = jnp.where(core == 0, ahead, back) * 2 + core
    frm = jnp.where(core == 0, back, ahead) * 2 + core
    mate = chip * 2 + 1 - core

    def part_of(k, b):
        return (x_ref if k == 0 else held.at[2 * k]).at[pl.ds(b * half, half)]

    def hop(k, b):
        return pltpu.make_async_remote_copy(
            src_ref=part_of(k, b), dst_ref=held.at[2 * k + 2, pl.ds(b * half, half)],
            send_sem=next_send.at[k, b], recv_sem=next_recv.at[k, b], device_id={"vp": to}, device_id_type=MESH)

    def swap(k, b):
        return pltpu.make_async_remote_copy(
            src_ref=part_of(k, b), dst_ref=held.at[2 * k + 1, pl.ds(b * half, half)],
            send_sem=swap_send.at[k, b], recv_sem=swap_recv.at[k, b], device_id={"vp": mate}, device_id_type=MESH)

    def keep(k):
        return pltpu.make_async_copy(held.at[k], all_ref.at[k], out_sem.at[k])

    @pl.when((s == 0) & (j == 0))
    def _():
        sem = pltpu.get_barrier_semaphore()
        for peer in (to, frm, mate):
            pl.semaphore_signal(sem, inc=1, device_id={"vp": peer}, device_id_type=MESH)
        pl.semaphore_wait(sem, 3)
        own = pltpu.make_async_copy(x_ref, held.at[0], in_sem)
        own.start()
        for b in range(2):
            swap(0, b).start()
            hop(0, b).start()
        own.wait()

    for k in range(chips):
        @pl.when((s == k) & (j == 0))
        def _():
            for b in range(2):
                swap(k, b).wait_recv()
            keep(2 * k).start()
            keep(2 * k + 1).start()

        if k < chips - 1:
            for b, when in ((0, steps // 2), (1, steps - 1)):
                @pl.when((s == k) & (j == when))
                def _():
                    hop(k, b).wait_recv()
                    if k < chips - 2:
                        hop(k + 1, b).start()
                    swap(k + 1, b).start()

    @pl.when(j == 0)
    def _():
        max_s[...] = jnp.full(max_s.shape, LOWEST, F32)
        sum_s[...] = jnp.zeros(sum_s.shape, F32)
        tail_s[...] = jnp.full(tail_s.shape, -jnp.inf, F32)

    limit = lim_ref[0]

    def gather(z):
        z = z.reshape(z.shape[0] // 8, 8, z.shape[1])
        old = max_s[...]
        new = jnp.maximum(old, jnp.max(z, axis=0))
        max_s[...] = new
        sum_s[...] = sum_s[...] * jnp.exp(old - new) + jnp.sum(jnp.exp(z - new[None]), axis=0)

    a = held[pl.ds(2 * s, 2)].reshape(2 * rows, depth)
    gather(tail_s[...])
    row0 = 0
    for i, part in enumerate(parts):
        z = lax.dot_general(w_ref[row0:row0 + part, :], a, (((1,), (1,)), ((), ())), preferred_element_type=F32)
        row = lax.broadcasted_iota(jnp.int32, z.shape, 0) + (j * tile + row0)
        z = jnp.where(row < limit, z, -jnp.inf)
        z_ref[row0:row0 + part, :] = z
        if i < len(parts) - 1:
            gather(z)
        else:
            tail_s[...] = z
        row0 += part

    @pl.when(j == steps - 1)
    def _():
        gather(tail_s[...])
        top = jnp.max(max_s[...], axis=0, keepdims=True)
        total = jnp.sum(sum_s[...] * jnp.exp(max_s[...] - top), axis=0, keepdims=True)
        st_ref[...] = jnp.where(lax.broadcasted_iota(jnp.int32, st_ref.shape, 0) == 0, top, total)

    @pl.when((s == chips - 1) & (j == steps - 1))
    def _():
        for k in range(chips):
            for b in range(2):
                if k < chips - 1:
                    hop(k, b).wait_send()
                swap(k, b).wait_send()
            keep(2 * k).wait()
            keep(2 * k + 1).wait()


def logits_call(limit, normed, wt, n, most=704):
    rows, depth = normed.shape
    chips = n // 2
    cols = wt.shape[0]
    tile = row_tile(cols, most)
    first = tile // 32 * 16
    sems = pltpu.SemaphoreType.DMA
    return pl.pallas_call(
        functools.partial(logits_kernel, n=n, parts=(tile - first, first)),
        grid=(chips, -(-cols // tile)),
        in_specs=[
            pl.BlockSpec(memory_space=pltpu.SMEM),
            pl.BlockSpec(memory_space=pl.ANY),
            pl.BlockSpec((tile, depth), lambda s, j: (j, 0)),
        ],
        out_specs=[
            pl.BlockSpec((None, tile, 2 * rows), lambda s, j: (s, j, 0)),
            pl.BlockSpec((None, 8, 2 * rows), lambda s, j: (s, 0, 0)),
            pl.BlockSpec(memory_space=pl.ANY),
        ],
        out_shape=[
            jax.ShapeDtypeStruct((chips, cols, 2 * rows), F32),
            jax.ShapeDtypeStruct((chips, 8, 2 * rows), F32),
            jax.ShapeDtypeStruct((n, rows, depth), BF16),
        ],
        scratch_shapes=[
            pltpu.VMEM((n, rows, depth), BF16),
            pltpu.VMEM((8, 2 * rows), F32),
            pltpu.VMEM((8, 2 * rows), F32),
            pltpu.VMEM((first, 2 * rows), F32),
            sems((chips - 1, 2)), sems((chips - 1, 2)), sems((chips, 2)), sems((chips, 2)), sems, sems((n,)),
        ],
        compiler_params=pltpu.CompilerParams(vmem_limit_bytes=VMEM_BYTES, collective_id=0, has_side_effects=True),
        cost_estimate=pl.CostEstimate(
            flops=2 * n * rows * depth * cols, bytes_accessed=chips * depth * cols * 2 + n * rows * cols * 4,
            transcendentals=n * rows * cols),
        name="logits",
    )(limit, normed, wt)


def stats_kernel(n, *refs):
    chips = n // 2
    st_ref, lw_ref = refs[:2]
    out_refs = refs[2:chips + 2]
    loss_ref, send, recv, table, send_sem, recv_sem = refs[chips + 2:]
    me = lax.axis_index("vp")
    core = lax.rem(me, 2)
    rows = lw_ref.shape[1]
    for step in range(chips):
        for half, block in enumerate(slot_block(me, core, step, chips)):
            span = pl.ds(half * rows, rows)
            send[pl.ds(block, 1), :] = st_ref[step, 0:1, span]
            send[pl.ds(n + block, 1), :] = st_ref[step, 1:2, span]
    send[2 * n:2 * n + 8, :] = lw_ref[...]
    barrier_all(me, n)
    share(me, n, send, recv, send_sem, recv_sem)
    top = recv[0, 0:n, :]
    for i in range(1, n):
        top = jnp.maximum(top, recv[i, 0:n, :])
    total = jnp.zeros_like(top)
    for i in range(n):
        total = total + recv[i, n:2 * n, :] * jnp.exp(recv[i, 0:n, :] - top)
    log_norm = top + jnp.log(total)
    labels = jnp.concatenate([recv[i, 2 * n:2 * n + 1, :] for i in range(n)], axis=0)
    weights = jnp.concatenate([recv[i, 2 * n + 1:2 * n + 2, :] for i in range(n)], axis=0)
    scale = weights / jnp.sum(jnp.sum(weights, axis=1, keepdims=True), axis=0, keepdims=True)
    loss = jnp.sum(jnp.sum(scale * log_norm, axis=1, keepdims=True), axis=0, keepdims=True)
    loss_ref[...] = jnp.broadcast_to(loss, loss_ref.shape)
    table[0:n, :] = log_norm
    table[n:2 * n, :] = scale
    table[2 * n:3 * n, :] = labels
    for step in range(chips):
        for half, block in enumerate(slot_block(me, core, step, chips)):
            for k in range(3):
                out_refs[step][k:k + 1, half * rows:(half + 1) * rows] = table[pl.ds(k * n + block, 1), :]


def stats_call(stats, label_weight, n):
    rows = label_weight.shape[1]
    vmem = pl.BlockSpec(memory_space=pltpu.VMEM)
    return pl.pallas_call(
        functools.partial(stats_kernel, n),
        in_specs=[vmem, vmem],
        out_specs=[vmem] * (n // 2 + 1),
        out_shape=[jax.ShapeDtypeStruct((8, 2 * rows), F32)] * (n // 2) + [jax.ShapeDtypeStruct((8, LANES), F32)],
        scratch_shapes=[
            pltpu.VMEM((2 * n + 8, rows), F32),
            pltpu.VMEM((n, 2 * n + 8, rows), F32),
            pltpu.VMEM((3 * n, rows), F32),
            pltpu.SemaphoreType.DMA((n - 1,)),
            pltpu.SemaphoreType.DMA((n - 1,)),
        ],
        compiler_params=pltpu.CompilerParams(collective_id=1, has_side_effects=True),
        cost_estimate=pl.CostEstimate(flops=4_000_000_000, bytes_accessed=n * rows * 512, transcendentals=0),
        name="stats",
    )(stats, label_weight)


def total_kernel(n, *refs):
    part_ref, loss_ref = refs[:2]
    hits = refs[2:-6]
    gain_ref, mean_ref, send, recv, send_sem, recv_sem = refs[-6:]
    me = lax.axis_index("vp")
    wide = send.shape[1]
    for r in range(8):
        send[r:r + 1, :] = part_ref[:, r * wide:(r + 1) * wide]
    hit = hits[0][...]
    for h in hits[1:]:
        hit = hit + h[...]
    send[8:16, :] = hit
    barrier_all(me, n)
    share(me, n, send, recv, send_sem, recv_sem)
    total = recv[0]
    for i in range(1, n):
        total = total + recv[i]
    for r in range(8):
        gain_ref[:, r * wide:(r + 1) * wide] = total[r:r + 1, :]
    target = jnp.sum(jnp.sum(total[8:16, :], axis=1, keepdims=True), axis=0, keepdims=True)
    mean_ref[...] = loss_ref[...] - target


def total_call(part, loss, hits, n):
    vmem = pl.BlockSpec(memory_space=pltpu.VMEM)
    buf = (16, hits[0].shape[1])
    return pl.pallas_call(
        functools.partial(total_kernel, n),
        in_specs=[vmem] * (len(hits) + 2),
        out_specs=[vmem, vmem],
        out_shape=[jax.ShapeDtypeStruct(part.shape, F32), jax.ShapeDtypeStruct(loss.shape, F32)],
        scratch_shapes=[
            pltpu.VMEM(buf, F32), pltpu.VMEM((n,) + buf, F32),
            pltpu.SemaphoreType.DMA((n - 1,)), pltpu.SemaphoreType.DMA((n - 1,))],
        compiler_params=pltpu.CompilerParams(collective_id=2, has_side_effects=True),
        cost_estimate=pl.CostEstimate(flops=4_000_000_000, bytes_accessed=part.size * 4 * n, transcendentals=0),
        name="total",
    )(part, loss, *hits)


def g_kernel(first_ref, row_ref, z_ref, w_ref, dzt_ref, gh_ref, gp_ref, hit_ref, *, cols, parts):
    j = pl.program_id(0)
    tile, tokens = z_ref.shape
    rows = tokens // 2
    last = pl.num_programs(0) - 1
    log_norm, scale = row_ref[0:1, :], row_ref[1:2, :]
    label = row_ref[2:3, :].astype(jnp.int32) - first_ref[0]
    label = jnp.where(label < cols, label, -1) - j * tile

    @pl.when(j == 0)
    def _():
        hit_ref[...] = jnp.zeros_like(hit_ref)
        gh_ref[...] = jnp.zeros_like(gh_ref)
        gp_ref[...] = jnp.zeros_like(gp_ref)

    def block(row0, count):
        z = z_ref[row0:row0 + count, :]
        is_target = lax.broadcasted_iota(jnp.int32, z.shape, 0) + row0 == label
        d = ((jnp.exp(z - log_norm) - jnp.where(is_target, 1.0, 0.0)) * scale).astype(BF16)
        dzt_ref[row0:row0 + count, :] = d
        hit_ref[...] += jnp.sum(jnp.where(is_target, z, 0.0).reshape(count // 8, 8, tokens), axis=0) * scale
        g = lax.dot_general(d, w_ref[row0:row0 + count, :], (((0,), (0,)), ((), ())), preferred_element_type=F32)
        gh_ref[...] += g[:rows]
        gp_ref[...] += g[rows:]

    rest = cols % tile
    if rest:
        @pl.when(j < last)
        def _():
            for k in range(parts):
                block(k * (tile // parts), tile // parts)

        @pl.when(j == last)
        def _():
            block(0, rest)
    else:
        for k in range(parts):
            block(k * (tile // parts), tile // parts)


def g_call(first_col, table, z, slot, wt, tile=512, parts=2):
    cols, tokens = z.shape[1:]
    depth = wt.shape[1]
    whole = pl.BlockSpec((tokens // 2, depth), lambda j: (0, 0))
    shape = jax.ShapeDtypeStruct((tokens // 2, depth), F32)
    return pl.pallas_call(
        functools.partial(g_kernel, cols=cols, parts=parts),
        grid=(-(-cols // tile),),
        in_specs=[
            pl.BlockSpec(memory_space=pltpu.SMEM),
            pl.BlockSpec((8, tokens), lambda j: (0, 0)),
            pl.BlockSpec((None, tile, tokens), lambda j: (slot, j, 0)),
            pl.BlockSpec((tile, depth), lambda j: (j, 0)),
        ],
        out_specs=[pl.BlockSpec((tile, tokens), lambda j: (j, 0)), whole, whole, pl.BlockSpec((8, tokens), lambda j: (0, 0))],
        out_shape=[jax.ShapeDtypeStruct((cols, tokens), BF16), shape, shape, jax.ShapeDtypeStruct((8, tokens), F32)],
        compiler_params=pltpu.CompilerParams(vmem_limit_bytes=VMEM_BYTES),
        cost_estimate=pl.CostEstimate(
            flops=2 * tokens * cols * depth, bytes_accessed=depth * cols * 2 + tokens * depth * 4 + tokens * cols * 6,
            transcendentals=tokens * cols),
        name="gmm",
    )(first_col, table, z, wt)


def dw_kernel(a_ref, *refs, chunks):
    out_ref = refs[-1]
    a = a_ref[...].reshape(-1, a_ref.shape[-1])
    dz = jnp.concatenate([r[...] for r in refs[:chunks]], axis=1)
    out_ref[...] = jnp.dot(dz, a, preferred_element_type=F32)


def dw_call(a, dz_chunks, start, count, previous=None, wide=1024, most=704):
    n, rows, depth = a.shape
    cols, chunk = dz_chunks[0].shape
    tile = row_tile(cols, most)
    base = start // wide
    specs = [pl.BlockSpec((n, rows, wide), lambda i, j: (0, 0, i + base))]
    specs += [pl.BlockSpec((tile, chunk), lambda i, j: (j, 0))] * len(dz_chunks)
    args = [a] + list(dz_chunks)
    aliases = {}
    if previous is not None:
        aliases = {len(args): 0}
        specs.append(pl.BlockSpec(memory_space=pl.ANY))
        args.append(previous)
    tokens = chunk * len(dz_chunks)
    return pl.pallas_call(
        functools.partial(dw_kernel, chunks=len(dz_chunks)),
        grid=(count // wide, -(-cols // tile)),
        in_specs=specs,
        out_specs=pl.BlockSpec((tile, wide), lambda i, j: (j, i + base)),
        out_shape=jax.ShapeDtypeStruct((cols, depth), F32),
        input_output_aliases=aliases,
        compiler_params=pltpu.CompilerParams(vmem_limit_bytes=VMEM_BYTES),
        cost_estimate=pl.CostEstimate(
            flops=2 * tokens * count * cols, bytes_accessed=count * cols * 4 + tokens * cols * 2, transcendentals=0),
        name="dunembed",
    )(*args)


def input_kernel(own_ref, other_ref, moved_ref, x_ref, gain_ref, dh_ref, part_ref, sums):
    i = pl.program_id(0)
    rows, depth = x_ref.shape
    g = own_ref[...] + other_ref[...] + moved_ref[...]
    x = x_ref[...].astype(F32)
    inv_rms = lax.rsqrt(jnp.mean(x * x, axis=-1, keepdims=True) + NORM_EPS)
    x_norm = x * inv_rms
    u = g * gain_ref[...]
    dh_ref[...] = (inv_rms * (u - x_norm * jnp.mean(u * x_norm, axis=-1, keepdims=True))).astype(BF16)
    part = jnp.sum((g * x_norm).reshape(rows // 8, 8, depth), axis=0)

    @pl.when(i == 0)
    def _():
        sums[...] = part

    @pl.when(i > 0)
    def _():
        sums[...] += part

    @pl.when(i == pl.num_programs(0) - 1)
    def _():
        part_ref[...] = jnp.sum(sums[...], axis=0, keepdims=True)


def input_call(own, other, moved, hidden, gain, tile=64):
    rows, depth = hidden.shape
    row = pl.BlockSpec((tile, depth), lambda i: (i, 0))
    whole = pl.BlockSpec((1, depth), lambda i: (0, 0))
    return pl.pallas_call(
        input_kernel,
        grid=(rows // tile,),
        in_specs=[row] * 4 + [whole],
        out_specs=[row, whole],
        out_shape=[jax.ShapeDtypeStruct((rows, depth), BF16), jax.ShapeDtypeStruct((1, depth), F32)],
        scratch_shapes=[pltpu.VMEM((8, depth), F32)],
        compiler_params=pltpu.CompilerParams(vmem_limit_bytes=VMEM_BYTES),
        cost_estimate=pl.CostEstimate(flops=8_000_000_000, bytes_accessed=rows * depth * 16, transcendentals=rows),
        name="dinput",
    )(own, other, moved, hidden, gain.reshape(1, depth))


def solution(mesh):
    n = mesh.shape["vp"]
    chips = n // 2
    swap = [(i, i ^ 1) for i in range(n)]
    ring = []
    for i in range(n):
        chip, core = i // 2, i % 2
        ring.append((i, ((chip + 1 if core == 0 else chip - 1) % chips) * 2 + core))

    def send(x, to):
        return lax.ppermute(x, "vp", to)

    def after(x, y):
        return lax.optimization_barrier((x, y))[0]

    def local_step(hidden, labels, loss_weight, norm_gain, w_local):
        rows, depth = hidden.shape
        cols = w_local.shape[1]
        wt = w_local.T
        first = lax.axis_index("vp") * cols
        limit = jnp.minimum(cols, cols * n - PAD_COLS - first).reshape(1)
        x_float = hidden.astype(F32)
        inv_rms = lax.rsqrt(jnp.mean(x_float * x_float, axis=-1, keepdims=True) + NORM_EPS)
        x_norm = x_float * inv_rms
        normed = (x_norm * norm_gain).astype(BF16)
        logits, stats, a_all = logits_call(limit, normed, wt, n)
        label_weight = jnp.zeros((8, rows), F32).at[0].set(labels.astype(F32)).at[1].set(loss_weight)
        *tables, loss_a = stats_call(stats, label_weight, n)
        order = list(range(1, chips)) + [0]
        dz_t, hits, grads = {}, [], {}
        for s in order:
            dz_t[s], own_part, other_part, hit = g_call(first.reshape(1), tables[s], logits, s, wt)
            hits.append(hit)
            grads[s] = (own_part, send(other_part, swap))
        dzs = [dz_t[s] for s in range(chips)]
        early = depth // 4
        moving = None
        for i, s in enumerate(order):
            own_part, other_part = grads[s]
            if s == 0:
                break
            acc = own_part + other_part
            if i > 0:
                acc = acc + moving
            moving = send(acc, ring)
            if i == 0:
                moving = after(moving, (hits[1], hits[2]))
            if i == chips - 3:
                d_unembed = dw_call(a_all, dzs, 0, early)
                moving, d_unembed = lax.optimization_barrier((moving, d_unembed))
            if i == chips - 2:
                d_unembed = dw_call(a_all, dzs, early, depth - early, d_unembed)
                moving, d_unembed = lax.optimization_barrier((moving, d_unembed))
        d_unembed = d_unembed.T
        d_input, part = input_call(own_part, other_part, moving, hidden, norm_gain)
        d_norm_gain, mean_loss = total_call(part, loss_a, hits, n)
        d_norm_gain = d_norm_gain.reshape(depth)
        mean_loss = mean_loss[0, :1]
        return mean_loss, d_input, d_unembed, d_norm_gain

    return jax.shard_map(
        local_step,
        mesh=mesh,
        in_specs=(P(("dp", "vp"), None), P(("dp", "vp")), P(("dp", "vp")), P(None), P(None, "vp")),
        out_specs=(P("dp"), P(("dp", "vp"), None), P("dp", "vp"), P("dp")),
        check_vma=False,
    )
```
